32 devices in a mesh: row: 4 (over y, x), col: 4 (over z), depth: 2 (over core).
Axes of the slice: x: 2, y: 2, z: 4, core: 2. Of those that a mesh axis runs over, the one named last changes fastest.
Arguments:
- layers: float32 [2, 4096, 4096], P('depth', 'row', 'col'), may hold values from -3 to 134.2, as said below
Outputs:
- factor: float32 [2, 4096, 512], P(None, 'row', 'depth')
- schur: float32 [4096, 4096], P(('row', 'depth'), 'col')
The draws below stay inside these ranges and needn't reach their ends.
Inputs may be any that keep to these rules, and one draw needn't show every extreme that they name: Read in matrix order, each layer is symmetric, and the sum over layers is symmetric positive definite with a diagonal of order sqrt(4096).
All inputs are finite; a program needn't handle non-finite values.
Results may differ from the reference program's by a relative error of at most 0.0001.
Values sent between devices are 32-bit elements; how exact they have to be, the bound alone decides.
A program may use at most 192 MiB of HBM per device.

```python
import jax
import jax.numpy as jnp
from jax import lax

PANEL = 512
BLOCKS_DEV = 2
PANELS = 2
LAYERS = 2
ORDER = 4096
COL_BLOCKS = 2
N_ROW = 4
N_COL = 4


def draw_layers(key, part):
    row_groups = ORDER // (PANEL * BLOCKS_DEV)
    col_groups = ORDER // (PANEL * COL_BLOCKS)
    positions = jnp.arange(ORDER, dtype=jnp.float32)
    distance = jnp.abs(positions[:, None] - positions[None, :])

    def one_layer(layer_index):
        layer_key = jax.random.fold_in(key, layer_index)
        noise_key, diag_key, scale_key, amp_key, reach_key = jax.random.split(layer_key, 5)
        noise = jnp.clip(jax.random.normal(noise_key, (ORDER, ORDER), jnp.float32), -4.0, 4.0)
        reach = PANEL * jax.random.uniform(reach_key, (), jnp.float32, 0.04, 0.12)
        amplitude = ORDER ** 0.5 * jax.random.uniform(amp_key, (), jnp.float32, 0.2, 0.45)
        symmetric = (noise + noise.T) * (0.5 / 1.4142135)
        row_scale = jax.random.uniform(scale_key, (ORDER,), jnp.float32, 0.7, 1.3)
        kernel = amplitude * row_scale[:, None] * row_scale[None, :] * jnp.exp(-distance / reach)
        diag_values = ORDER ** 0.5 * jax.random.uniform(diag_key, (ORDER,), jnp.float32, 0.75, 1.25)
        matrix = symmetric + kernel + jnp.diag(diag_values)
        rows = matrix.reshape(BLOCKS_DEV, row_groups, PANEL, ORDER).transpose(1, 0, 2, 3).reshape(ORDER, ORDER)
        return rows.reshape(ORDER, COL_BLOCKS, col_groups, PANEL).transpose(0, 2, 1, 3).reshape(ORDER, ORDER)
    return lax.map(one_layer, jnp.arange(LAYERS, dtype=jnp.int32)).astype(jnp.float32)


def setup_inputs(seed: int = 0) -> dict:
    streams_of = jax.random.split(jax.random.key(seed), 2)
    layers = draw_layers(jax.random.fold_in(streams_of[1], 71), 0)
    return dict(layers=layers)


def to_matrix(array):
    rows = array.reshape(N_ROW, BLOCKS_DEV, PANEL, ORDER).transpose(1, 0, 2, 3).reshape(ORDER, ORDER)
    return rows.reshape(ORDER, N_COL, COL_BLOCKS, PANEL).transpose(0, 2, 1, 3).reshape(ORDER, ORDER)

def rows_to_storage(matrix):
    width = matrix.shape[1]
    return matrix.reshape(BLOCKS_DEV, N_ROW, PANEL, width).transpose(1, 0, 2, 3).reshape(ORDER, width)

def to_storage(matrix):
    rows = rows_to_storage(matrix)
    return rows.reshape(ORDER, COL_BLOCKS, N_COL, PANEL).transpose(0, 2, 1, 3).reshape(ORDER, ORDER)

def reference(layers):
    matrix = to_matrix(jnp.sum(layers, axis=0))
    identity_block = jnp.eye(PANEL, dtype=jnp.float32)
    columns = []
    for panel_step in range(PANELS):
        first = panel_step * PANEL
        after = first + PANEL
        lower_diag = jnp.linalg.cholesky(matrix[first:after, first:after])
        inverse = jax.scipy.linalg.solve_triangular(lower_diag, identity_block, lower=True)
        solved = jnp.dot(matrix[first:, first:after], inverse.T, precision=lax.Precision.HIGHEST)
        column = jnp.concatenate([jnp.zeros((first, PANEL), jnp.float32), solved], axis=0)
        columns.append(rows_to_storage(column))
        below = solved[PANEL:]
        update = jnp.dot(below, below.T, precision=lax.Precision.HIGHEST)
        matrix = matrix.at[after:, after:].add(-update)
    return (jnp.stack(columns), to_storage(matrix))
```

```python
import functools

import jax
import jax.numpy as jnp
from jax import lax
from jax.experimental import pallas as pl
from jax.experimental.pallas import tpu as pltpu
from jax.sharding import PartitionSpec as P

PANEL = 512
PANELS = 2
INNER = 128
STRIP = 8
HIGH = lax.Precision.HIGH
HIGHEST = lax.Precision.HIGHEST


def dot(a, b, ca, cb, precision):
    return lax.dot_general(
        a, b, (((ca,), (cb,)), ((), ())), precision=precision, preferred_element_type=jnp.float32
    )


def factor_strip(work, inv, strip):
    first = pl.multiple_of(strip * STRIP, STRIP)
    rows = work[pl.ds(first, STRIP), :]
    irows = inv[pl.ds(first, STRIP), :]
    rolled = pltpu.roll(rows, (INNER - first) % INNER, 1)
    sub = lax.broadcasted_iota(jnp.int32, (STRIP, INNER), 0)
    lane = lax.broadcasted_iota(jnp.int32, (STRIP, INNER), 1)
    cols = [jnp.broadcast_to(rolled[:, t : t + 1], (STRIP, INNER)) for t in range(STRIP)]
    pivots = jnp.zeros((STRIP, INNER), jnp.float32)
    for t in range(STRIP):
        pivot = jnp.broadcast_to(cols[t][t : t + 1, :], (STRIP, INNER))
        pivots = jnp.where(sub == t, pivot, pivots)
        if t + 1 < STRIP:
            mult = jnp.where(sub > t, cols[t] * (1.0 / pivot), 0.0)
            for s in range(t + 1, STRIP):
                cols[s] = cols[s] - mult * jnp.broadcast_to(cols[s][t : t + 1, :], (STRIP, INNER))
            rows = rows - mult * jnp.broadcast_to(rows[t : t + 1, :], (STRIP, INNER))
            irows = irows - mult * jnp.broadcast_to(irows[t : t + 1, :], (STRIP, INNER))
    scale = lax.rsqrt(pivots)
    rows = rows * scale
    irows = irows * scale
    inv[pl.ds(first, STRIP), :] = irows
    below = jnp.where(lane >= first + STRIP, rows, 0.0)
    update = dot(below, jnp.concatenate([rows, irows], axis=1), 0, 0, HIGHEST)
    work[...] -= update[:, :INNER]
    inv[...] -= update[:, INNER:]


def inverse_kernel(block_ref, out_ref, whole, work, inv):
    size = block_ref.shape[0]
    whole[...] = block_ref[...]
    eye = (
        lax.broadcasted_iota(jnp.int32, (INNER, INNER), 0)
        == lax.broadcasted_iota(jnp.int32, (INNER, INNER), 1)
    ).astype(jnp.float32)
    out_ref[...] = jnp.zeros_like(out_ref)
    for k in range(size // INNER):
        lo, hi = k * INNER, (k + 1) * INNER
        work[...] = whole[lo:hi, lo:hi]
        inv[...] = eye

        def step(strip, carry):
            factor_strip(work, inv, strip)
            return carry

        lax.fori_loop(0, INNER // STRIP, step, 0)
        corner = inv[...]
        if k:
            out_ref[lo:hi, :lo] = dot(corner, out_ref[lo:hi, :lo], 1, 0, HIGHEST)
        out_ref[lo:hi, lo:hi] = corner
        if hi < size:
            below = dot(whole[hi:, lo:hi], corner, 1, 1, HIGHEST)
            whole[hi:, hi:] -= dot(below, below, 1, 1, HIGHEST)
            out_ref[hi:, :hi] -= dot(below, out_ref[lo:hi, :hi], 1, 0, HIGHEST)


def block_inverse(block):
    size = block.shape[0]
    return pl.pallas_call(
        inverse_kernel,
        out_shape=jax.ShapeDtypeStruct((size, size), jnp.float32),
        in_specs=[pl.BlockSpec(memory_space=pltpu.VMEM)],
        out_specs=pl.BlockSpec(memory_space=pltpu.VMEM),
        scratch_shapes=[
            pltpu.VMEM((size, size), jnp.float32),
            pltpu.VMEM((INNER, INNER), jnp.float32),
            pltpu.VMEM((INNER, INNER), jnp.float32),
        ],
        cost_estimate=pl.CostEstimate(flops=2 * size**3, bytes_accessed=8 * size**2, transcendentals=size),
        name="block_inverse",
    )(block)


def pick(index, table):
    value = 0
    for i, entry in enumerate(table):
        value = value + jnp.where(index == i, entry, 0)
    return value


def spread_kernel(groups, s_ref, rowp, colp, diag, zrecv, zsend, rrecv, rsend, srecv, ssend, lsem):
    row_groups, col_groups = groups
    r, c, d = lax.axis_index("row"), lax.axis_index("col"), lax.axis_index("depth")
    z_chunks, chunks = zrecv.shape[1], rrecv.shape[1]
    ring = list(range(row_groups))
    if row_groups & (row_groups - 1) == 0:
        ring = [i ^ (i >> 1) for i in ring]
    place = [ring.index(i) for i in range(row_groups)]
    pos = pick(r, place)
    after = pick(r, [ring[(place[i] + 1) % row_groups] for i in range(row_groups)])
    before = pick(r, [ring[(place[i] - 1) % row_groups] for i in range(row_groups)])
    target = jnp.where(d == 0, after, before)
    half = PANEL // 2
    last = []

    def local(src, dst):
        copy = pltpu.make_async_copy(src, dst, lsem)
        copy.start()
        copy.wait()

    def line(p, k):
        root, lane = p % col_groups, (p // col_groups) * PANEL
        size = PANEL // z_chunks
        rows = pl.ds(k * size, size)
        block = rowp.at[p, rows]

        def copy(way):
            return pltpu.make_async_remote_copy(
                src_ref=block,
                dst_ref=block,
                send_sem=zsend.at[p, k, max(way, 0)],
                recv_sem=zrecv.at[p, k],
                device_id={"col": c + way},
                device_id_type=pl.DeviceIdType.MESH,
            )

        @pl.when(c == root)
        def _():
            local(s_ref.at[rows, pl.ds(lane, PANEL)], block)

        @pl.when(c != root)
        def _():
            copy(1).wait_recv()

        up, down = (c >= root) & (c < col_groups - 1), (c <= root) & (c > 0)

        @pl.when(up)
        def _():
            copy(1).start()

        @pl.when(down)
        def _():
            copy(-1).start()

        def finish():
            @pl.when(up)
            def _():
                copy(1).wait_send()

            @pl.when(down)
            def _():
                copy(-1).wait_send()

        last.append(finish)

    def around(item, root, owner, src, dst, k):
        start = place[root]
        rel = jnp.where(d == 0, (pos - start + row_groups) % row_groups, (start - pos + row_groups) % row_groups)
        size = half // chunks
        own = pl.ds(pl.multiple_of(d * half + k * size, size), size)
        other = pl.ds(pl.multiple_of((1 - d) * half + k * size, size), size)
        is_root = rel == 0
        sends = rel < row_groups - 1
        origin = is_root & (d == owner)

        def hop():
            return pltpu.make_async_remote_copy(
                src_ref=dst.at[own],
                dst_ref=dst.at[own],
                send_sem=rsend.at[item, k],
                recv_sem=rrecv.at[item, k],
                device_id={"row": target},
                device_id_type=pl.DeviceIdType.MESH,
            )

        def across(kind):
            block = dst.at[(own, other)[kind]]
            return pltpu.make_async_remote_copy(
                src_ref=block,
                dst_ref=block,
                send_sem=ssend.at[item, kind, k],
                recv_sem=srecv.at[item, kind, k],
                device_id={"depth": 1 - d},
                device_id_type=pl.DeviceIdType.MESH,
            )

        @pl.when(origin)
        def _():
            local(src.at[other], dst.at[other])
            across(1).start()
            local(src.at[own], dst.at[own])
            across(0).start()

        @pl.when(is_root & (d != owner))
        def _():
            across(1).wait_recv()

        @pl.when(rel > 0)
        def _():
            hop().wait_recv()

        @pl.when(sends)
        def _():
            hop().start()

        @pl.when(rel > 0)
        def _():
            across(0).start()

        def finish():
            @pl.when(origin)
            def _():
                across(1).wait_send()
                across(0).wait_send()

            @pl.when(jnp.logical_not(origin))
            def _():
                across(0).wait_recv()

            @pl.when(rel > 0)
            def _():
                across(0).wait_send()

            @pl.when(sends)
            def _():
                hop().wait_send()

        last.append(finish)

    def owner_of(p):
        return p % row_groups, p // row_groups

    pairs = [(p, q) for p in range(PANELS) for q in range(p + 1)]
    order = [k for j in range(z_chunks // 2) for k in (j, j + z_chunks // 2)]
    for p in range(PANELS):
        for j in range(max(z_chunks, chunks)):
            if j < z_chunks:
                line(p, order[j])
            if j < chunks:
                around(len(pairs) + p, *owner_of(p), s_ref, colp.at[p], j)
        for item, (a, b) in enumerate(pairs):
            if b == p:
                for k in range(chunks):
                    around(item, *owner_of(a), rowp.at[b], diag.at[item], k)
    for finish in last:
        finish()


def spread(summed, row_groups, col_groups):
    cols = summed.shape[1]
    z_chunks, chunks = 4, 4
    blocks = PANELS * (PANELS + 1) // 2
    items = blocks + PANELS
    dma = pltpu.SemaphoreType.DMA
    vmem = pl.BlockSpec(memory_space=pltpu.VMEM)
    return pl.pallas_call(
        functools.partial(spread_kernel, (row_groups, col_groups)),
        out_shape=(
            jax.ShapeDtypeStruct((PANELS, PANEL, PANEL), jnp.float32),
            jax.ShapeDtypeStruct((PANELS, PANEL, cols), jnp.float32),
            jax.ShapeDtypeStruct((blocks, PANEL, PANEL), jnp.float32),
        ),
        in_specs=[vmem],
        out_specs=(vmem, vmem, vmem),
        scratch_shapes=[
            dma((PANELS, z_chunks)),
            dma((PANELS, z_chunks, 2)),
            dma((items, chunks)),
            dma((items, chunks)),
            dma((items, 2, chunks)),
            dma((items, 2, chunks)),
            dma,
        ],
        compiler_params=pltpu.CompilerParams(has_side_effects=True, vmem_limit_bytes=60 * 1024 * 1024),
        name="spread",
    )(summed)


def per_device(layers):
    row_groups = lax.axis_size("row")
    col_groups = lax.axis_size("col")
    depth_groups = lax.axis_size("depth")
    row = lax.axis_index("row")
    col = lax.axis_index("col")
    depth = lax.axis_index("depth")
    layer = layers[0]
    cols_local = layer.shape[1]
    assert layer.shape[0] == PANEL * depth_groups and depth_groups == 2

    swap = [(0, 1), (1, 0)]
    mine = lax.dynamic_slice_in_dim(layer, depth * PANEL, PANEL, 0)
    theirs = lax.dynamic_slice_in_dim(layer, (1 - depth) * PANEL, PANEL, 0)
    summed = mine + lax.ppermute(theirs, "depth", swap)
    own_block = row + row_groups * depth
    col_block = jnp.arange(cols_local, dtype=jnp.int32) // PANEL * col_groups + col

    rowp, colp, diag = spread(summed, row_groups, col_groups)
    rows = [rowp[p] for p in range(PANELS)]
    cols = [colp[p] for p in range(PANELS)]
    pairs = [(p, q) for p in range(PANELS) for q in range(p + 1)]
    lead = {pair: diag[i] for i, pair in enumerate(pairs)}
    factors, left, right = [], [], []
    for p in range(PANELS):
        inverse = block_inverse(lead[p, p])
        solved = {a: dot(lead[a, p], inverse, 1, 1, HIGHEST) for a in range(p + 1, PANELS)}
        for a in range(p + 1, PANELS):
            for b in range(p + 1, a + 1):
                lead[a, b] = lead[a, b] - dot(solved[a], solved[b], 1, 1, HIGHEST)
        c_rows = jnp.where(own_block >= p, dot(rows[p], inverse, 1, 1, HIGH), 0.0)
        below = jnp.where(own_block > p, c_rows, 0.0)
        c_cols = dot(inverse, cols[p], 1, 0, HIGH)
        c_cols = jnp.where((col_block > p)[None, :], c_cols, 0.0)
        factors.append(c_rows)
        left.append(below)
        right.append(c_cols)
        for q in range(p + 1, PANELS):
            rows[q] = rows[q] - dot(below, solved[q], 1, 1, HIGH)
            cols[q] = cols[q] - dot(solved[q], c_cols, 1, 0, HIGH)
    update = dot(jnp.concatenate(left, 1), jnp.concatenate(right, 0), 1, 0, HIGH)
    schur = summed - update
    factor = jnp.stack(factors)
    width = PANEL // depth_groups
    kept = lax.dynamic_slice_in_dim(factor, depth * width, width, 2)
    sent = lax.dynamic_slice_in_dim(factor, (1 - depth) * width, width, 2)
    got = lax.ppermute(sent, "depth", swap)
    first = jnp.where(depth == 0, kept, got)
    second = jnp.where(depth == 0, got, kept)
    return jnp.concatenate([first, second], axis=1), schur


def solution(mesh):
    return jax.shard_map(
        per_device,
        mesh=mesh,
        in_specs=(P("depth", "row", "col"),),
        out_specs=(P(None, "row", "depth"), P(("row", "depth"), "col")),
        check_vma=False,
    )
```
